32 devices in a mesh: gx: 4 (over y, x), gy: 8 (over z, core).
Axes of the slice: x: 2, y: 2, z: 4, core: 2. Of those that a mesh axis runs over, the one named last changes fastest.
Arguments:
- schur_blocks: float32 [32, 2048, 2048], P(('gx', 'gy')), may hold values from -1 to 11, as said below
- offsets: int32 [32], P(('gx', 'gy')), may hold values from 256 to 768, as said below
- right_side: float32 [32768, 128], P(('gx', 'gy')), may hold values from -20 to 20
- coarse_basis: float32 [32768, 128], P(('gx', 'gy')), may hold values from -0.03125 to 0.03125
- coarse_load: float32 [128, 128], replicated, may hold values from -6 to 6
Outputs:
- multipliers: float32 [32768, 128], P(('gx', 'gy'))
- amplitudes: float32 [128, 128], replicated
The draws below stay inside these ranges and needn't reach their ends.
Inputs may be any that keep to these rules, and one draw needn't show every extreme that they name: `schur_blocks`: each block is symmetric positive definite. `offsets`: both ends of the range are taken by some subdomain.
All inputs are finite; a program needn't handle non-finite values.
Results may differ from the reference program's by a relative error of at most 0.0003.
Values sent between devices are 32-bit elements; how exact they have to be, the bound alone decides.
No kernel may reach another device: no remote copies, remote signals or barrier semaphores. Data moves between devices by JAX's collectives and lax.ppermute only.
A program may use at most 128 MiB of HBM per device.

```python
import math
import jax
import jax.numpy as jnp
from jax import lax

W = 2048
SLAB = 1024
R = 128
NC = 128
ITERS = 3
SUBDOMAINS = 32
MULTS = 32768


def draw_schur_blocks(key, part):
    upper_end = 4.0
    subkeys = jax.random.split(key, SUBDOMAINS)

    def single(subkey):
        diag_key, noise_key = jax.random.split(subkey)
        diagonal = jnp.exp(jax.random.uniform(diag_key, (W,), jnp.float32, 0.0, math.log(upper_end)))
        noise_part = jax.random.truncated_normal(noise_key, -5.0, 5.0, (W, W), jnp.float32) * (0.25 / math.sqrt(W))
        return jnp.diag(diagonal) + (noise_part + noise_part.T) * 0.7071067811865476
    return lax.map(single, subkeys)


def draw_offsets(key, part):
    key_values, key_ranking = jax.random.split(key)
    lowest = SLAB // 4
    highest = 3 * SLAB // 4
    values = jax.random.randint(key_values, (SUBDOMAINS,), lowest, highest + 1).astype(jnp.int32)
    ranking = jax.random.permutation(key_ranking, SUBDOMAINS)
    values = values.at[ranking[0]].set(lowest).at[ranking[1]].set(highest)
    return values.astype(jnp.int32)


def draw_right_side(key, part):
    base_key = jax.random.fold_in(key, 0)
    total_rows = SLAB * SUBDOMAINS
    position = jnp.arange(total_rows, dtype=jnp.float32) / total_rows
    base = jax.random.truncated_normal(base_key, -4.0, 4.0, (total_rows, R), jnp.float32)
    rising = 1.0 + 2.0 * position
    return base * rising[:, None]


def block_scale(stream_key, dims, cuts, low, top_value):
    gain, own = 1.0, jax.random.fold_in(stream_key, 6)
    for dim, shards_of in cuts:
        heights = jnp.exp(jax.random.uniform(jax.random.fold_in(own, dim), (shards_of,), jnp.float32, low / len(cuts), top_value / len(cuts)))
        gain = gain * jnp.repeat(heights, dims[dim] // shards_of).reshape([-1 if axis == dim else 1 for axis in range(len(dims))])
    return gain


def gaussian(stream_key, extent, spread, reach, pieces=(), kind=jnp.bfloat16):
    values = jax.random.normal(stream_key, extent, jnp.float32) * spread
    if len(pieces) > 0:
        values = block_scale(stream_key, extent, pieces, -0.22, 0.18) * values
    return jnp.clip(values, min=-reach, max=reach).astype(kind)


def setup_inputs(seed: int = 0) -> dict:
    keys = jax.random.split(jax.random.key(seed), 6)
    return {
        "schur_blocks": draw_schur_blocks(jax.random.fold_in(keys[5], 71), 0),
        "offsets": draw_offsets(jax.random.fold_in(keys[5], 71), 0),
        "right_side": draw_right_side(jax.random.fold_in(keys[5], 71), 0),
        "coarse_basis": gaussian(keys[3], (MULTS, NC), MULTS ** -0.5, 0.03125, ((0, 32),), jnp.float32),
        "coarse_load": gaussian(keys[4], (NC, R), 1.0, 6.0, (), jnp.float32),
    }


HIGHEST = lax.Precision.HIGHEST

def apply_operator(vector, schur_blocks, offsets):
    padded = jnp.pad(vector, ((SLAB, SLAB), (0, 0)))

    def visit_block(accumulated, inputs):
        schur_block, start_row, device_index = inputs
        first_row = (device_index * SLAB + start_row).astype(jnp.int32)
        window = lax.dynamic_slice_in_dim(padded, first_row, W, 0)
        product_block = jnp.dot(schur_block.astype(jnp.float32), window.astype(jnp.float32), precision=HIGHEST, preferred_element_type=jnp.float32)
        current = lax.dynamic_slice_in_dim(accumulated, first_row, W, 0)
        return (lax.dynamic_update_slice_in_dim(accumulated, current + product_block, first_row, 0), None)
    indices = jnp.arange(SUBDOMAINS, dtype=jnp.int32)
    accumulated, _ = lax.scan(visit_block, jnp.zeros_like(padded), (schur_blocks, offsets.astype(jnp.int32), indices))
    return accumulated[SLAB:SLAB + vector.shape[0]]

def project(residual, coarse_basis, gram_factor):
    coarse_part = jnp.dot(coarse_basis.T.astype(jnp.float32), residual.astype(jnp.float32), precision=HIGHEST, preferred_element_type=jnp.float32)
    amplitudes = jax.scipy.linalg.cho_solve((gram_factor, True), coarse_part)
    projected = residual - jnp.dot(coarse_basis.astype(jnp.float32), amplitudes.astype(jnp.float32), precision=HIGHEST, preferred_element_type=jnp.float32)
    return (projected, amplitudes)

def reference(schur_blocks, offsets, right_side, coarse_basis, coarse_load):
    gram_matrix = jnp.dot(coarse_basis.T.astype(jnp.float32), coarse_basis.astype(jnp.float32), precision=HIGHEST, preferred_element_type=jnp.float32)
    gram_factor = jnp.linalg.cholesky(gram_matrix)
    start_load = jax.scipy.linalg.cho_solve((gram_factor, True), coarse_load)
    multipliers = jnp.dot(coarse_basis.astype(jnp.float32), start_load.astype(jnp.float32), precision=HIGHEST, preferred_element_type=jnp.float32)
    residual = right_side - apply_operator(multipliers, schur_blocks, offsets)
    projected, amplitudes = project(residual, coarse_basis, gram_factor)
    direction = projected
    energy_now = jnp.sum(projected * projected, axis=0)
    for iteration in range(ITERS):
        operator_image = apply_operator(direction, schur_blocks, offsets)
        step_length = energy_now / jnp.sum(direction * operator_image, axis=0)
        multipliers = multipliers + step_length * direction
        residual = residual - step_length * operator_image
        projected, amplitudes = project(residual, coarse_basis, gram_factor)
        energy_next = jnp.sum(projected * projected, axis=0)
        direction = projected + energy_next / energy_now * direction
        energy_now = energy_next
    return (multipliers, amplitudes)
```

```python
import jax
import jax.numpy as jnp
from jax import lax
from jax.experimental import pallas as pl
from jax.experimental.pallas import tpu as pltpu
from jax.sharding import PartitionSpec as P

ITERS = 3
AXES = ("gx", "gy")
HIGHEST = lax.Precision.HIGHEST
F32 = jnp.float32
BF16 = jnp.bfloat16
BLOCK = 256
MIB = 1 << 20


def dot(a, b):
    return jnp.dot(a, b, precision=HIGHEST, preferred_element_type=F32)


def dot_t(a, b):
    return lax.dot_general(
        a, b, (((0,), (0,)), ((), ())), precision=HIGHEST, preferred_element_type=F32
    )


def all_sum(value):
    count = lax.axis_size(AXES)
    bit = 1
    while bit < count:
        pairs = [(i, i ^ bit) for i in range(count)]
        value = value + lax.ppermute(value, AXES, pairs)
        bit *= 2
    return value


def swap(first, second):
    count = lax.axis_size(AXES)
    even, odd = [], []
    for i in range(0, count - 1, 2):
        even += [(i, i + 1), (i + 1, i)]
    for i in range(1, count - 1, 2):
        odd += [(i, i + 1), (i + 1, i)]
    return lax.ppermute(first, AXES, even), lax.ppermute(second, AXES, odd)


def fold(x):
    return jnp.sum(x.reshape(x.shape[0] // 8, 8, x.shape[1]), axis=0)


def total(x):
    return jnp.sum(x, axis=0, keepdims=True)


def product_kernel(meta, block, own, recv_e, recv_o, p_own, p_e, p_o, win, prod, quad, ext, cat, pext):
    step = pl.program_id(0)
    steps = pl.num_programs(0)
    slab, cols = own.shape
    reach = recv_e.shape[0]
    start = meta[0]
    even = meta[1]
    right = reach + slab
    e_at = pl.multiple_of(even * right, 8)
    o_at = pl.multiple_of((1 - even) * right, 8)
    rows = block.shape[1]

    @pl.when(step == 0)
    def _():
        ext[pl.ds(e_at, reach), :] = recv_e[...]
        ext[pl.ds(o_at, reach), :] = recv_o[...]
        ext[reach:right, :] = own[...]
        pext[...] = jnp.zeros(pext.shape, F32)
        quad[...] = jnp.zeros(quad.shape, F32)
        for j in range(win.shape[0] // BLOCK):
            chunk = ext[pl.ds(start + j * BLOCK, BLOCK), :]
            high = chunk.astype(BF16)
            low = (chunk - high.astype(F32)).astype(BF16)
            win[j * BLOCK : (j + 1) * BLOCK, :] = chunk
            cat[j * BLOCK : (j + 1) * BLOCK, :cols] = high
            cat[j * BLOCK : (j + 1) * BLOCK, cols:] = low

    a = block[0]
    a_high = a.astype(BF16)
    a_low = (a - a_high.astype(F32)).astype(BF16)
    wide = jnp.dot(a_high, cat[...], preferred_element_type=F32)
    narrow = jnp.dot(a_low, cat[:, :cols], preferred_element_type=F32)
    out = wide[:, :cols] + (wide[:, cols:] + narrow)
    at = pl.multiple_of(step * rows, rows)
    prod[pl.ds(at, rows), :] = out
    pext[pl.ds(start + at, rows), :] = out
    here = win[pl.ds(at, rows), :]
    if quad.shape[0] == 8:
        quad[...] += fold(here * out)
    else:
        quad[...] += dot_t(here, out)

    @pl.when(step == steps - 1)
    def _():
        p_own[...] = pext[reach:right, :]
        p_e[...] = pext[pl.ds(e_at, reach), :]
        p_o[...] = pext[pl.ds(o_at, reach), :]


def whole(shape):
    return pl.BlockSpec(shape, lambda *_: (0,) * len(shape))


def product(meta, schur, own, recv_e, recv_o, quad_rows):
    slab, cols = own.shape
    reach = recv_e.shape[0]
    window = schur.shape[1]
    span = 2 * reach + slab
    rows = BLOCK
    vec = lambda n: jax.ShapeDtypeStruct((n, cols), F32)
    outs = (vec(slab), vec(reach), vec(reach), vec(window), vec(window), vec(quad_rows))
    return pl.pallas_call(
        product_kernel,
        grid_spec=pltpu.PrefetchScalarGridSpec(
            num_scalar_prefetch=1,
            grid=(window // rows,),
            in_specs=[
                pl.BlockSpec((1, rows, window), lambda i, m: (0, i, 0)),
                whole((slab, cols)),
                whole((reach, cols)),
                whole((reach, cols)),
            ],
            out_specs=[whole(o.shape) for o in outs],
            scratch_shapes=[
                pltpu.VMEM((span, cols), F32),
                pltpu.VMEM((window, 2 * cols), BF16),
                pltpu.VMEM((span, cols), F32),
            ],
        ),
        out_shape=outs,
        compiler_params=pltpu.CompilerParams(
            dimension_semantics=("arbitrary",), vmem_limit_bytes=24 * MIB
        ),
        cost_estimate=pl.CostEstimate(
            flops=8 * window * window * cols, bytes_accessed=4 * window * window, transcendentals=0
        ),
        name="product",
    )(meta, schur, own, recv_e, recv_o)


def call(kernel, meta, args, shapes, name, limit=16):
    outs = tuple(jax.ShapeDtypeStruct(s, F32) for s in shapes)
    vmem = pl.BlockSpec(memory_space=pltpu.VMEM)
    return pl.pallas_call(
        kernel,
        in_specs=[pl.BlockSpec(memory_space=pltpu.SMEM)] + [vmem] * len(args),
        out_specs=[vmem] * len(outs),
        out_shape=outs,
        compiler_params=pltpu.CompilerParams(vmem_limit_bytes=limit * MIB),
        name=name,
    )(meta, *args)


def places(meta, slab, reach):
    base = slab - reach
    even = meta[1]
    return pl.multiple_of(even * base, 8), pl.multiple_of((1 - even) * base, 8)


def gather_rows(meta, dst, p_own, recv_e, recv_o):
    slab, reach = p_own.shape[0], recv_e.shape[0]
    e_at, o_at = places(meta, slab, reach)
    dst[...] = p_own[...]
    dst[pl.ds(e_at, reach), :] += recv_e[...]
    dst[pl.ds(o_at, reach), :] += recv_o[...]


def offer(meta, src, send_e, send_o):
    slab, reach = src.shape[0], send_e.shape[0]
    e_at, o_at = places(meta, slab, reach)
    send_e[...] = src[pl.ds(e_at, reach), :]
    send_o[...] = src[pl.ds(o_at, reach), :]


def begin_kernel(meta, basis, rhs, send_e, send_o, sums):
    nc = basis.shape[1]
    offer(meta, basis, send_e, send_o)
    b = basis[...]
    sums[:nc, :] = dot_t(b, b)
    sums[nc:, :] = dot_t(b, rhs[...])


def start_kernel(meta, p_own, recv_e, recv_o, basis, rhs, m_sum, b_sum, inverse, load,
                 c, lam, u, send_e, send_o, rho, sums):
    gather_rows(meta, c, p_own, recv_e, recv_o)
    y = dot(inverse[...], load[...])
    coarse = b_sum[...] - dot(m_sum[...], y)
    amp = dot(inverse[...], coarse)
    rho[...] = coarse
    lam[...] = dot(basis[...], y)
    u[...] = rhs[...] - dot(c[...], y) - dot(basis[...], amp)
    offer(meta, u, send_e, send_o)
    nc = basis.shape[1]
    sums[:nc, :] = dot_t(c[...], u[...])
    sums[nc:, :] = fold(u[...] * u[...])


def image_kernel(meta, p_own, recv_e, recv_o, c, w, send_e, send_o, more):
    gather_rows(meta, w, p_own, recv_e, recv_o)
    offer(meta, w, send_e, send_o)
    more[...] = dot_t(c[...], w[...])


def first_kernel(meta, p_own, recv_e, recv_o, basis, c, inverse, sums, u, w, lam, rho,
                 w1, send_e, send_o, lam1, u1, q0, rho1, amp0, scal, out):
    nc = basis.shape[1]
    gather_rows(meta, w1, p_own, recv_e, recv_o)
    k0 = sums[:nc, :]
    a0 = dot(inverse[...], k0)
    gamma = total(sums[2 * nc : 2 * nc + 8, :])
    curve = total(sums[2 * nc + 8 : 2 * nc + 16, :])
    alpha = gamma / curve
    w1[...] = w[...] - alpha * (w1[...] - dot(c[...], a0))
    offer(meta, w1, send_e, send_o)
    q0[...] = w[...] - dot(basis[...], a0)
    u1[...] = u[...] - alpha * q0[...]
    lam1[...] = lam[...] + alpha * u[...]
    rho1[...] = rho[...] - alpha * k0
    amp0[...] = a0
    scal[0:1, :] = gamma
    scal[1:2, :] = curve
    scal[2:3, :] = alpha
    scal[3:8, :] = jnp.zeros((5, scal.shape[1]), F32)
    out[:nc, :] = dot_t(c[...], u1[...])
    out[nc : 2 * nc, :] = dot_t(c[...], w1[...])
    out[2 * nc : 2 * nc + 8, :] = fold(u1[...] * u1[...])
    out[2 * nc + 8 : 2 * nc + 16, :] = fold(u1[...] * w1[...])
    out[2 * nc + 16 :, :] = fold(u1[...] * w[...])


def windows_kernel(meta, u_win, w_win, b_win, pu, pw, pb, amp0, scal, u1_win, q0_win, pu1, pq0):
    a0 = amp0[...]
    alpha = scal[2:3, :]
    q0_win[...] = w_win[...] - dot(b_win[...], a0)
    u1_win[...] = u_win[...] - alpha * q0_win[...]
    pq0[...] = pw[...] - dot(pb[...], a0)
    pu1[...] = pu[...] - alpha * pq0[...]


def second_kernel(meta, sums, inverse, m_sum, basis, u0, w0, w1, u1, q0, lam1, rho1, sums0, amp0, scal,
                  u1_win, q0_win, pu1, pq0, w1_win, pw1, b_win, pb,
                  lam2, u2, p1, rho2, k2, kk1, scal2, out):
    nc = basis.shape[1]
    k1 = sums[:nc, :]
    l1 = sums[nc : 2 * nc, :]
    gamma1 = total(sums[2 * nc : 2 * nc + 8, :])
    delta1 = total(sums[2 * nc + 8 : 2 * nc + 16, :])
    eps1 = total(sums[2 * nc + 16 :, :])
    gamma0 = scal[0:1, :]
    curve0 = scal[1:2, :]
    beta = gamma1 / gamma0
    curve = delta1 + beta * (2.0 * eps1 + beta * curve0)
    alpha = gamma1 / curve
    a1 = dot(inverse[...], k1)
    k0 = sums0[:nc, :]
    l0 = sums0[nc : 2 * nc, :]
    q1_win = w1_win[...] - dot(b_win[...], a1) + beta * q0_win[...]
    pq1 = pw1[...] - dot(pb[...], a1) + beta * pq0[...]
    u2_win = u1_win[...] - alpha * q1_win
    pu2 = pu1[...] - alpha * pq1
    q1 = w1[...] - dot(basis[...], a1) + beta * q0[...]
    u2[...] = u1[...] - alpha * q1
    s1 = w1[...] + beta * w0[...]
    out[0:8, :] = fold(u2[...] * u2[...])
    out[8:16, :] = fold(u2_win * pu2)
    out[16:24, :] = fold(u2[...] * s1)
    p1[...] = u1[...] + beta * u0[...]
    lam2[...] = lam1[...] + alpha * p1[...]
    kk1[...] = k1 + beta * k0
    rho2[...] = rho1[...] - alpha * kk1[...]
    cq0 = l0 - dot(m_sum[...], amp0[...])
    k2[...] = k1 - alpha * (l1 - dot(m_sum[...], a1) + beta * cq0)
    scal2[0:1, :] = gamma1
    scal2[1:2, :] = curve
    scal2[2:8, :] = jnp.zeros((6, scal2.shape[1]), F32)


def last_kernel(meta, sums, inverse, lam2, u2, p1, rho2, k2, kk1, scal2, lam, amp):
    gamma2 = total(sums[0:8, :])
    delta2 = total(sums[8:16, :])
    eps2 = total(sums[16:24, :])
    beta = gamma2 / scal2[0:1, :]
    curve = delta2 + beta * (2.0 * eps2 + beta * scal2[1:2, :])
    alpha = gamma2 / curve
    lam[...] = lam2[...] + alpha * (u2[...] + beta * p1[...])
    rho3 = rho2[...] - alpha * (k2[...] + beta * kk1[...])
    amp[...] = dot(inverse[...], rho3)


def local(schur, offsets, rhs, basis, load):
    slab, cols = rhs.shape
    nc = basis.shape[1]
    window = schur.shape[1]
    reach = 3 * slab // 4
    index = lax.axis_index(AXES)
    meta = jnp.stack([offsets[0] - (slab - reach), 1 - index % 2]).astype(jnp.int32)
    vec, hal, sml = (slab, cols), (reach, cols), (nc, cols)
    win = (window, cols)

    send_e, send_o, sums = call(begin_kernel, meta, (basis, rhs), (hal, hal, (2 * nc, cols)), "begin")
    recv = swap(send_e, send_o)
    gram_rhs = all_sum(sums)
    p_own, p_e, p_o, b_win, pb, m_local = product(meta, schur, basis, *recv, nc)
    recv = swap(p_e, p_o)
    m_sum = all_sum(m_local)
    factor = jnp.linalg.cholesky(gram_rhs[:nc])
    tri = lax.linalg.triangular_solve(factor, jnp.eye(nc, dtype=F32), left_side=True, lower=True)
    inverse = dot_t(tri, tri)
    c, lam0, u0, send_e, send_o, rho0, sums = call(
        start_kernel, meta, (p_own, *recv, basis, rhs, m_sum, gram_rhs[nc:], inverse, load),
        (vec, vec, vec, hal, hal, sml, (nc + 8, cols)), "start")
    recv = swap(send_e, send_o)
    p_own, p_e, p_o, u_win, pu, delta = product(meta, schur, u0, *recv, 8)
    recv = swap(p_e, p_o)
    w0, send_e, send_o, more = call(
        image_kernel, meta, (p_own, *recv, c), (vec, hal, hal, sml), "image")
    recv = swap(send_e, send_o)
    sums0 = all_sum(jnp.concatenate([sums[:nc], more, sums[nc:], delta], axis=0))
    p_own, p_e, p_o, w_win, pw, _ = product(meta, schur, w0, *recv, 8)
    recv = swap(p_e, p_o)
    big = (2 * nc + 24, cols)
    w1, send_e, send_o, lam1, u1, q0, rho1, amp0, scal, sums = call(
        first_kernel, meta, (p_own, *recv, basis, c, inverse, sums0, u0, w0, lam0, rho0),
        (vec, hal, hal, vec, vec, vec, sml, sml, (8, cols), big), "first")
    recv = swap(send_e, send_o)
    sums1 = all_sum(sums)
    u1_win, q0_win, pu1, pq0 = call(
        windows_kernel, meta, (u_win, w_win, b_win, pu, pw, pb, amp0, scal), (win,) * 4, "windows", 24)
    _, _, _, w1_win, pw1, _ = product(meta, schur, w1, *recv, 8)
    lam2, u2, p1, rho2, k2, kk1, scal2, sums = call(
        second_kernel, meta,
        (sums1, inverse, m_sum, basis, u0, w0, w1, u1, q0, lam1, rho1, sums0, amp0, scal,
         u1_win, q0_win, pu1, pq0, w1_win, pw1, b_win, pb),
        (vec, vec, vec, sml, sml, sml, (8, cols), (24, cols)), "second", 40)
    sums2 = all_sum(sums)
    lam, amp = call(
        last_kernel, meta, (sums2, inverse, lam2, u2, p1, rho2, k2, kk1, scal2), (vec, sml), "last")
    return lam, amp


def solution(mesh):
    in_specs = (P(AXES, None, None), P(AXES), P(AXES, None), P(AXES, None), P())
    out_specs = (P(AXES, None), P())
    return jax.shard_map(local, mesh=mesh, in_specs=in_specs, out_specs=out_specs, check_vma=False)
```

```python
import jax
import jax.numpy as jnp
from jax import lax
from jax.experimental import pallas as pl
from jax.experimental.pallas import tpu as pltpu
from jax.sharding import PartitionSpec as P


AXES = ("gx", "gy")
HIGHEST = lax.Precision.HIGHEST
F32 = jnp.float32
BF16 = jnp.bfloat16
BLOCK = 256
MIB = 1 << 20


def dot(a, b):
    return jnp.dot(a, b, precision=HIGHEST, preferred_element_type=F32)


def dot_t(a, b):
    return lax.dot_general(
        a, b, (((0,), (0,)), ((), ())), precision=HIGHEST, preferred_element_type=F32
    )


def exchange_sum(value, bits):
    count = lax.axis_size(AXES)
    masks = [0]
    for bit in bits:
        masks += [mask | bit for mask in masks]
    out = value
    for mask in masks[1:]:
        out = out + lax.ppermute(value, AXES, [(j, j ^ mask) for j in range(count)])
    return out


def groups(count):
    bits = [1 << i for i in range(1, count.bit_length() - 1)]
    return [bits[i : i + 2] for i in range(0, len(bits), 2)][::-1]


def core_sum(value):
    return exchange_sum(value, [1])


def core_swap(value):
    count = lax.axis_size(AXES)
    return lax.ppermute(value, AXES, [(i, i ^ 1) for i in range(count)])


def far_sum(value):
    for group in groups(lax.axis_size(AXES))[:-1]:
        value = exchange_sum(value, group)
    return value


def near_sum(value):
    last = groups(lax.axis_size(AXES))[-1]
    return exchange_sum(value, last)


def swap(first, second):
    count = lax.axis_size(AXES)
    even, odd = [], []
    for i in range(0, count - 1, 2):
        even += [(i, i + 1), (i + 1, i)]
    for i in range(1, count - 1, 2):
        odd += [(i, i + 1), (i + 1, i)]
    second = lax.ppermute(second, AXES, odd)
    first = lax.ppermute(first, AXES, even)
    return first, second


def fold(x):
    return jnp.sum(x.reshape(x.shape[0] // 8, 8, x.shape[1]), axis=0)


def total(x):
    return jnp.sum(x, axis=0, keepdims=True)


def in_vmem():
    return pl.BlockSpec(memory_space=pltpu.VMEM)


def pack(win, cat, cols):
    for j in range(win.shape[0] // BLOCK):
        chunk = win[j * BLOCK : (j + 1) * BLOCK, :]
        high = chunk.astype(BF16)
        cat[j * BLOCK : (j + 1) * BLOCK, :cols] = high
        cat[j * BLOCK : (j + 1) * BLOCK, cols:] = (chunk - high.astype(F32)).astype(BF16)


def load_window(meta, own, recv_e, recv_o, ext, win, cat):
    put(meta, own, recv_e, recv_o, ext)
    for j in range(win.shape[0] // BLOCK):
        win[j * BLOCK : (j + 1) * BLOCK, :] = ext[pl.ds(meta[0] + j * BLOCK, BLOCK), :]
    pack(win, cat, own.shape[1])


def multiply(a_high, a_low, cat, cols):
    wide = jnp.dot(a_high, cat[...], preferred_element_type=F32)
    narrow = jnp.dot(a_low, cat[:, :cols], preferred_element_type=F32)
    return wide[:, :cols] + (wide[:, cols:] + narrow)


def hand_out(meta, pext, p_own, p_e, p_o):
    slab, reach = p_own.shape[0], p_e.shape[0]
    right = reach + slab
    p_own[...] = pext[reach:right, :]
    p_e[...] = pext[pl.ds(pl.multiple_of(meta[1] * right, 8), reach), :]
    p_o[...] = pext[pl.ds(pl.multiple_of((1 - meta[1]) * right, 8), reach), :]


def split_kernel(block, a_high, a_low):
    rows = block.shape[1]
    at = pl.multiple_of(pl.program_id(0) * rows, rows)
    a = block[0]
    high = a.astype(BF16)
    a_high[pl.ds(at, rows), :] = high
    a_low[pl.ds(at, rows), :] = (a - high.astype(F32)).astype(BF16)


def split(schur):
    window = schur.shape[1]
    rows = BLOCK
    return pl.pallas_call(
        split_kernel,
        grid=(window // rows,),
        in_specs=[pl.BlockSpec((1, rows, window), lambda i: (0, i, 0))],
        out_specs=[in_vmem()] * 2,
        out_shape=(jax.ShapeDtypeStruct((window, window), BF16),) * 2,
        compiler_params=pltpu.CompilerParams(
            dimension_semantics=("arbitrary",), vmem_limit_bytes=8 * MIB
        ),
        cost_estimate=pl.CostEstimate(
            flops=8 * window * window * 128, bytes_accessed=8 * window * window, transcendentals=0
        ),
        name="split",
    )(pltpu.with_memory_space_constraint(schur, pltpu.HBM))


def put(meta, own, recv_e, recv_o, ext):
    slab, reach = own.shape[0], recv_e.shape[0]
    right = reach + slab
    ext[pl.ds(pl.multiple_of(meta[1] * right, 8), reach), :] = recv_e[...]
    ext[pl.ds(pl.multiple_of((1 - meta[1]) * right, 8), reach), :] = recv_o[...]
    ext[reach:right, :] = own[...]


def product_kernel(meta, a_high, a_low, own, recv_e, recv_o, *rest):
    ext, win, cat, pext = rest[-4:]
    cols = own.shape[1]
    load_window(meta, own, recv_e, recv_o, ext, win, cat)
    spread(meta, a_high, a_low, win, cat, pext, rest[:-4], cols)


def spread(meta, a_high, a_low, win, cat, pext, outs, cols):
    if len(outs) > 1:
        pext[...] = jnp.zeros(pext.shape, F32)
    else:
        outs[0][...] = jnp.zeros(outs[0].shape, F32)

    def step(j, carry):
        at = pl.multiple_of(j * BLOCK, BLOCK)
        out = multiply(a_high[pl.ds(at, BLOCK), :], a_low[pl.ds(at, BLOCK), :], cat, cols)
        if len(outs) > 1:
            pext[pl.ds(meta[0] + at, BLOCK), :] = out
        else:
            outs[0][...] += fold(win[pl.ds(at, BLOCK), :] * out)
        return carry

    lax.fori_loop(0, win.shape[0] // BLOCK, step, 0)
    if len(outs) > 1:
        hand_out(meta, pext, *outs)


def product(meta, a_high, a_low, parts, outgoing):
    slab, cols = parts[0].shape
    reach = parts[1].shape[0]
    window = a_high.shape[0]
    span = 2 * reach + slab
    vec = lambda n: jax.ShapeDtypeStruct((n, cols), F32)
    outs = (vec(slab), vec(reach), vec(reach)) if outgoing else (vec(8),)
    return pl.pallas_call(
        product_kernel,
        in_specs=[pl.BlockSpec(memory_space=pltpu.SMEM)] + [in_vmem()] * (2 + len(parts)),
        out_specs=[in_vmem()] * len(outs),
        scratch_shapes=[
            pltpu.VMEM((span, cols), F32),
            pltpu.VMEM((window, cols), F32),
            pltpu.VMEM((window, 2 * cols), BF16),
            pltpu.VMEM((span, cols), F32),
        ],
        out_shape=outs,
        compiler_params=pltpu.CompilerParams(vmem_limit_bytes=12 * MIB),
        cost_estimate=pl.CostEstimate(
            flops=8 * window * window * cols, bytes_accessed=4 * window * window, transcendentals=0
        ),
        name="product",
    )(meta, a_high, a_low, *parts)


def call(kernel, meta, args, shapes, limit=8):
    outs = tuple(jax.ShapeDtypeStruct(s, F32) for s in shapes)
    return pl.pallas_call(
        kernel,
        in_specs=[pl.BlockSpec(memory_space=pltpu.SMEM)] + [in_vmem()] * len(args),
        out_specs=[in_vmem()] * len(outs),
        out_shape=outs,
        compiler_params=pltpu.CompilerParams(vmem_limit_bytes=limit * MIB),
    )(meta, *args)


def places(meta, slab, reach):
    base = slab - reach
    even = meta[1]
    return pl.multiple_of(even * base, 8), pl.multiple_of((1 - even) * base, 8)


def gather_rows(meta, dst, p_own, recv_e, recv_o):
    slab, reach = p_own.shape[0], recv_e.shape[0]
    e_at, o_at = places(meta, slab, reach)
    dst[...] = p_own[...]
    dst[pl.ds(e_at, reach), :] += recv_e[...]
    dst[pl.ds(o_at, reach), :] += recv_o[...]


def offer(meta, src, send_e, send_o):
    slab, reach = src.shape[0], send_e.shape[0]
    e_at, o_at = places(meta, slab, reach)
    send_e[...] = src[pl.ds(e_at, reach), :]
    send_o[...] = src[pl.ds(o_at, reach), :]


def begin_kernel(meta, basis, send_e, send_o, keep, give):
    n = basis.shape[1]
    offer(meta, basis, send_e, send_o)
    gram = dot_t(basis[...], basis[...])
    share(meta, gram[: n // 2, :], gram[n // 2 :, :], keep, give)


def inverse_kernel(meta, mine, other, load, inv, y):
    n = inv.shape[0]
    inv[: n // 2, :], inv[n // 2 :, :] = shared(meta, mine[...], other[...])
    lane = lax.broadcasted_iota(jnp.int32, (1, n), 1)
    lanes = lax.broadcasted_iota(jnp.int32, (n, n), 1)

    def pick(row, k):
        return jnp.sum(jnp.where(lane == k, row, 0.0), axis=1, keepdims=True)

    def step(j, carry):
        k = 2 * j
        m = inv[...]
        col_a = jnp.sum(jnp.where(lanes == k, m, 0.0), axis=1, keepdims=True)
        col_b = jnp.sum(jnp.where(lanes == k + 1, m, 0.0), axis=1, keepdims=True)
        row_a = inv[pl.ds(k, 1), :]
        row_b = inv[pl.ds(k + 1, 1), :]
        a, b, d = pick(row_a, k), pick(row_a, k + 1), pick(row_b, k + 1)
        schur = d - b * (b / a)
        row_a = jnp.where(lane == k, 1.0, jnp.where(lane == k + 1, 0.0, row_a))
        row_b = jnp.where(lane == k, 0.0, jnp.where(lane == k + 1, 1.0, row_b))
        new_b = (row_b - (b / a) * row_a) / schur
        new_a = (row_a - b * new_b) / a
        m = jnp.where((lanes == k) | (lanes == k + 1), 0.0, m)
        inv[...] = m - col_a * new_a - col_b * new_b
        inv[pl.ds(k, 1), :] = new_a
        inv[pl.ds(k + 1, 1), :] = new_b
        return carry

    lax.fori_loop(0, n // 2, step, 0)
    y[...] = dot(inv[...], load[...])


def start_kernel(meta, p_own, recv_e, recv_o, rhs, y, c, r, send_e, send_o):
    gather_rows(meta, c, p_own, recv_e, recv_o)
    r[...] = rhs[...] - dot(c[...], y[...])
    offer(meta, r, send_e, send_o)


def share(meta, first, second, keep, give):
    n = first.shape[0]
    even = meta[1] == 1
    keep[:n, :] = jnp.where(even, first, second)
    give[:n, :] = jnp.where(even, second, first)


def shared(meta, mine, other):
    even = meta[1] == 1
    return jnp.where(even, mine, other), jnp.where(even, other, mine)


def pair_rows(meta, scalars, keep, give, n):
    even = meta[1] == 1
    keep[n:, :] = jnp.zeros((8, keep.shape[1]), F32)
    give[n:, :] = jnp.zeros((8, give.shape[1]), F32)
    for i, row in enumerate(scalars):
        keep[n + i : n + i + 1, :] = jnp.where(even, row, 0.0)
        give[n + i : n + i + 1, :] = jnp.where(even, 0.0, row)


def coarse_kernel(meta, basis, rhs, c, keep, give):
    share(meta, dot_t(basis[...], c[...]), dot_t(basis[...], rhs[...]), keep, give)


def amp_kernel(meta, mine, other, inverse, y, m, rho, amp):
    m_sum, b_sum = shared(meta, mine[...], other[...])
    coarse = b_sum - dot(m_sum, y[...])
    m[...] = m_sum
    rho[...] = coarse
    amp[...] = dot(inverse[...], coarse)


def image_kernel(meta, p_own, recv_e, recv_o, c, amp, w, send_e, send_o):
    gather_rows(meta, w, p_own, recv_e, recv_o)
    w[...] = w[...] - dot(c[...], amp[...])
    offer(meta, w, send_e, send_o)


def sums_kernel(meta, c, r, y, basis, amp, w, u, keep, give, lam):
    n = basis.shape[1]
    lam[...] = dot(basis[...], y[...])
    u[...] = r[...] - dot(basis[...], amp[...])
    share(meta, dot_t(c[...], u[...]), dot_t(c[...], w[...]), keep, give)
    pair_rows(meta, [total(u[...] * u[...]), total(u[...] * w[...])], keep, give, n)


def amp0_kernel(meta, mine, other, inverse, m, k0, a0, cq0, scal):
    n = inverse.shape[0]
    first, second = shared(meta, mine[...], other[...])
    amp = dot(inverse[...], first[:n, :])
    k0[...] = first[:n, :]
    a0[...] = amp
    cq0[...] = second[:n, :] - dot(m[...], amp)
    scal[...] = first[n:, :]


def first_kernel(meta, p_own, recv_e, recv_o, c, a0, scal, w, w1, send_e, send_o):
    gather_rows(meta, w1, p_own, recv_e, recv_o)
    alpha = scal[0:1, :] / scal[1:2, :]
    w1[...] = w[...] - alpha * (w1[...] - dot(c[...], a0[...]))
    offer(meta, w1, send_e, send_o)


def sums1_kernel(meta, basis, c, a0, k0, scal, u, w, lam, rho, p_own, recv_e, recv_o, w1,
                 lam1, u1, q0, rho1, keep, give, n0):
    n = basis.shape[1]
    gather_rows(meta, n0, p_own, recv_e, recv_o)
    alpha = scal[0:1, :] / scal[1:2, :]
    n0[...] = n0[...] - dot(c[...], a0[...])
    q0[...] = w[...] - dot(basis[...], a0[...])
    u1[...] = u[...] - alpha * q0[...]
    lam1[...] = lam[...] + alpha * u[...]
    rho1[...] = rho[...] - alpha * k0[...]
    share(meta, dot_t(c[...], u1[...]), dot_t(c[...], w1[...]), keep, give)
    pairs = ((u1, u1), (u1, w1), (u1, q0), (w1, w1), (w1, q0), (q0, q0), (n0, w1), (n0, q0))
    pair_rows(meta, [total(a[...] * b[...]) for a, b in pairs], keep, give, n)


def last_kernel(meta, mine, other, inverse, m, basis, u0, w1, u1, q0, lam1, rho1, k0, cq0, scal, lam, amp):
    n = inverse.shape[0]
    omega = total(mine[n + 8 :, :])
    first, second = shared(meta, mine[...], other[...])
    k1, l1 = first[:n, :], second[:n, :]
    uu, uw, uq, ww, wq, qq, nw, nq = (first[n + i : n + i + 1, :] for i in range(8))
    a1 = dot(inverse[...], k1)
    ma1 = dot(m[...], a1)
    beta = uu / scal[0:1, :]
    curve = uw + beta * (2.0 * uq + beta * scal[1:2, :])
    alpha = uu / curve
    mw = ww - total(a1 * k1)
    u_q1 = uw + beta * uq
    q1_q1 = mw + beta * (2.0 * wq + beta * qq)
    q1_w1 = mw + beta * wq
    m_n = nw - total(a1 * cq0[...])
    m_fm = omega + total(a1 * (ma1 - 2.0 * l1))
    q1_fq1 = m_fm + beta * (2.0 * m_n + beta * nq)
    gamma2 = uu + alpha * (alpha * q1_q1 - 2.0 * u_q1)
    delta2 = uw + alpha * (alpha * q1_fq1 - 2.0 * q1_w1)
    eps2 = u_q1 - alpha * q1_q1
    beta2 = gamma2 / uu
    p1 = u1[...] + beta * u0[...]
    q1 = w1[...] - dot(basis[...], a1) + beta * q0[...]
    curve2 = delta2 + beta2 * (2.0 * eps2 + beta2 * curve)
    alpha2 = gamma2 / curve2
    lam[...] = lam1[...] + alpha * p1 + alpha2 * (u1[...] - alpha * q1 + beta2 * p1)
    kk1 = k1 + beta * k0[...]
    k2 = k1 - alpha * (l1 - ma1 + beta * cq0[...])
    amp[...] = dot(inverse[...], rho1[...] - alpha * kk1 - alpha2 * (k2 + beta2 * kk1))


def steps(schur, offsets, rhs, basis, load):
    slab, cols = rhs.shape
    nc = basis.shape[1]
    reach = 3 * slab // 4
    index = lax.axis_index(AXES)
    meta = jnp.stack([offsets[0] - (slab - reach), 1 - index % 2]).astype(jnp.int32)
    vec, hal, sml = (slab, cols), (reach, cols), (nc, cols)
    rows8 = (8, cols)
    half = (nc + 8, cols)

    send_e, send_o, keep, give = call(
        begin_kernel, meta, (basis,), (hal, hal, (nc // 2, nc), (nc // 2, nc)))
    recv = swap(send_e, send_o)
    mine = near_sum(keep + core_swap(give))
    a_high, a_low = split(schur)
    mine = far_sum(mine)
    p_own, p_e, p_o = product(meta, a_high, a_low, (basis, *recv), True)
    recv = swap(p_e, p_o)
    other = core_swap(mine)
    inverse, y = call(inverse_kernel, meta, (mine, other, load), ((nc, nc), sml))
    c, r0, send_e, send_o = call(
        start_kernel, meta, (p_own, *recv, rhs, y), (vec, vec, hal, hal))
    recv = swap(send_e, send_o)
    keep, give = call(coarse_kernel, meta, (basis, rhs, c), (sml, sml))
    mine = near_sum(keep + core_swap(give))
    p_own, p_e, p_o = product(meta, a_high, a_low, (r0, *recv), True)
    recv = swap(p_e, p_o)
    mine = far_sum(mine)
    other = core_swap(mine)
    m, rho0, amp = call(amp_kernel, meta, (mine, other, inverse, y), (sml, sml, sml))
    w0, send_e, send_o = call(
        image_kernel, meta, (p_own, *recv, c, amp), (vec, hal, hal))
    recv = swap(send_e, send_o)
    u0, keep, give, lam0 = call(
        sums_kernel, meta, (c, r0, y, basis, amp, w0), (vec, half, half, vec))
    mine = near_sum(keep + core_swap(give))
    p_own, p_e, p_o = product(meta, a_high, a_low, (w0, *recv), True)
    recv = swap(p_e, p_o)
    mine = far_sum(mine)
    other = core_swap(mine)
    k0, a0, cq0, scal = call(
        amp0_kernel, meta, (mine, other, inverse, m), (sml, sml, sml, rows8))
    w1, send_e, send_o = call(
        first_kernel, meta, (p_own, *recv, c, a0, scal, w0), (vec, hal, hal))
    recv_in = swap(send_e, send_o)
    lam1, u1, q0, rho1, keep, give, _ = call(
        sums1_kernel, meta, (basis, c, a0, k0, scal, u0, w0, lam0, rho0, p_own, *recv, w1),
        (vec, vec, vec, sml, half, half, vec))
    mine = near_sum(keep + core_swap(give))
    (omega,) = product(meta, a_high, a_low, (w1, *recv_in), False)
    omega = near_sum(core_sum(omega))
    mine = far_sum(jnp.concatenate([mine, omega], axis=0))
    other = core_swap(mine)
    lam, amp = call(
        last_kernel, meta,
        (mine, other, inverse, m, basis, u0, w1, u1, q0, lam1, rho1, k0, cq0, scal),
        (vec, sml))
    return lam, amp


def solution(mesh):
    in_specs = (P(AXES, None, None), P(AXES), P(AXES, None), P(AXES, None), P())
    out_specs = (P(AXES, None), P())
    return jax.shard_map(steps, mesh=mesh, in_specs=in_specs, out_specs=out_specs, check_vma=False)
```

```python
import jax
import jax.numpy as jnp
from jax import lax
from jax.experimental import pallas as pl
from jax.experimental.pallas import tpu as pltpu
from jax.sharding import PartitionSpec as P


AXES = ("gx", "gy")
HIGHEST = lax.Precision.HIGHEST
F32 = jnp.float32
BF16 = jnp.bfloat16
BLOCK = 256
ROWS = 1024
MIB = 1 << 20


def dot(a, b):
    return jnp.dot(a, b, precision=HIGHEST, preferred_element_type=F32)


def dot_t(a, b):
    return lax.dot_general(
        a, b, (((0,), (0,)), ((), ())), precision=HIGHEST, preferred_element_type=F32
    )


def exchange_sum(value, bits):
    count = lax.axis_size(AXES)
    masks = [0]
    for bit in bits:
        masks += [mask | bit for mask in masks]
    out = value
    for mask in masks[1:]:
        out = out + lax.ppermute(value, AXES, [(j, j ^ mask) for j in range(count)])
    return out


def groups(count):
    bits = [1 << i for i in range(1, count.bit_length() - 1)]
    return [bits[i : i + 2] for i in range(0, len(bits), 2)][::-1]


def core_sum(value):
    return exchange_sum(value, [1])


def core_swap(value):
    count = lax.axis_size(AXES)
    return lax.ppermute(value, AXES, [(i, i ^ 1) for i in range(count)])


def far_sum(value):
    for group in groups(lax.axis_size(AXES))[:-1]:
        value = exchange_sum(value, group)
    return value


def near_sum(value):
    last = groups(lax.axis_size(AXES))[-1]
    return exchange_sum(value, last)


def swap(first, second):
    count = lax.axis_size(AXES)
    even, odd = [], []
    for i in range(0, count - 1, 2):
        even += [(i, i + 1), (i + 1, i)]
    for i in range(1, count - 1, 2):
        odd += [(i, i + 1), (i + 1, i)]
    second = lax.ppermute(second, AXES, odd)
    first = lax.ppermute(first, AXES, even)
    return first, second


def fold(x):
    return jnp.sum(x.reshape(x.shape[0] // 8, 8, x.shape[1]), axis=0)


def total(x):
    return jnp.sum(x, axis=0, keepdims=True)


def in_vmem():
    return pl.BlockSpec(memory_space=pltpu.VMEM)


def pack(win, cat, cols):
    for j in range(win.shape[0] // BLOCK):
        chunk = win[j * BLOCK : (j + 1) * BLOCK, :]
        high = chunk.astype(BF16)
        cat[j * BLOCK : (j + 1) * BLOCK, :cols] = high
        cat[j * BLOCK : (j + 1) * BLOCK, cols:] = (chunk - high.astype(F32)).astype(BF16)


def load_window(meta, own, recv_e, recv_o, ext, win, cat):
    put(meta, own, recv_e, recv_o, ext)
    for j in range(win.shape[0] // BLOCK):
        win[j * BLOCK : (j + 1) * BLOCK, :] = ext[pl.ds(meta[0] + j * BLOCK, BLOCK), :]
    pack(win, cat, own.shape[1])


def multiply(a_high, a_low, cat, cols):
    wide = jnp.dot(a_high, cat[...], preferred_element_type=F32)
    narrow = jnp.dot(a_low, cat[:, :cols], preferred_element_type=F32)
    return wide[:, :cols] + (wide[:, cols:] + narrow)


def hand_out(meta, pext, p_own, p_e, p_o):
    slab, reach = p_own.shape[0], p_e.shape[0]
    right = reach + slab
    p_own[...] = pext[reach:right, :]
    p_e[...] = pext[pl.ds(pl.multiple_of(meta[1] * right, 8), reach), :]
    p_o[...] = pext[pl.ds(pl.multiple_of((1 - meta[1]) * right, 8), reach), :]


def split_kernel(block, a_high, a_low):
    rows = block.shape[1]
    at = pl.multiple_of(pl.program_id(0) * rows, rows)
    a = block[0]
    high = a.astype(BF16)
    a_high[pl.ds(at, rows), :] = high
    a_low[pl.ds(at, rows), :] = (a - high.astype(F32)).astype(BF16)


def split(schur):
    window = schur.shape[1]
    rows = 2 * BLOCK
    return pl.pallas_call(
        split_kernel,
        grid=(window // rows,),
        in_specs=[pl.BlockSpec((1, rows, window), lambda i: (0, i, 0))],
        out_specs=[in_vmem()] * 2,
        out_shape=(jax.ShapeDtypeStruct((window, window), BF16),) * 2,
        compiler_params=pltpu.CompilerParams(
            dimension_semantics=("arbitrary",), vmem_limit_bytes=20 * MIB
        ),
        cost_estimate=pl.CostEstimate(
            flops=8 * window * window * 128, bytes_accessed=8 * window * window, transcendentals=0
        ),
        name="split",
    )(pltpu.with_memory_space_constraint(schur, pltpu.HBM))


def put(meta, own, recv_e, recv_o, ext):
    slab, reach = own.shape[0], recv_e.shape[0]
    right = reach + slab
    ext[pl.ds(pl.multiple_of(meta[1] * right, 8), reach), :] = recv_e[...]
    ext[pl.ds(pl.multiple_of((1 - meta[1]) * right, 8), reach), :] = recv_o[...]
    ext[reach:right, :] = own[...]


def product_kernel(meta, a_high, a_low, own, recv_e, recv_o, *rest):
    ext, win, cat, pext = rest[-4:]
    cols = own.shape[1]
    load_window(meta, own, recv_e, recv_o, ext, win, cat)
    spread(meta, a_high, a_low, win, cat, pext, rest[:-4], cols)


def spread(meta, a_high, a_low, win, cat, pext, outs, cols):
    if len(outs) > 1:
        pext[...] = jnp.zeros(pext.shape, F32)
    else:
        outs[0][...] = jnp.zeros(outs[0].shape, F32)

    def step(j, carry):
        at = pl.multiple_of(j * ROWS, ROWS)
        out = multiply(a_high[pl.ds(at, ROWS), :], a_low[pl.ds(at, ROWS), :], cat, cols)
        if len(outs) > 1:
            pext[pl.ds(meta[0] + at, ROWS), :] = out
        else:
            outs[0][...] += fold(win[pl.ds(at, ROWS), :] * out)
        return carry

    lax.fori_loop(0, win.shape[0] // ROWS, step, 0)
    if len(outs) > 1:
        hand_out(meta, pext, *outs)


def product(meta, a_high, a_low, parts, outgoing):
    slab, cols = parts[0].shape
    reach = parts[1].shape[0]
    window = a_high.shape[0]
    span = 2 * reach + slab
    vec = lambda n: jax.ShapeDtypeStruct((n, cols), F32)
    outs = (vec(slab), vec(reach), vec(reach)) if outgoing else (vec(8),)
    return pl.pallas_call(
        product_kernel,
        in_specs=[pl.BlockSpec(memory_space=pltpu.SMEM)] + [in_vmem()] * (2 + len(parts)),
        out_specs=[in_vmem()] * len(outs),
        scratch_shapes=[
            pltpu.VMEM((span, cols), F32),
            pltpu.VMEM((window, cols), F32),
            pltpu.VMEM((window, 2 * cols), BF16),
            pltpu.VMEM((span, cols), F32),
        ],
        out_shape=outs,
        compiler_params=pltpu.CompilerParams(vmem_limit_bytes=20 * MIB),
        cost_estimate=pl.CostEstimate(
            flops=8 * window * window * cols, bytes_accessed=4 * window * window, transcendentals=0
        ),
        name="product",
    )(meta, a_high, a_low, *parts)


def call(kernel, meta, args, shapes, limit=8):
    outs = tuple(jax.ShapeDtypeStruct(s, F32) for s in shapes)
    return pl.pallas_call(
        kernel,
        in_specs=[pl.BlockSpec(memory_space=pltpu.SMEM)] + [in_vmem()] * len(args),
        out_specs=[in_vmem()] * len(outs),
        out_shape=outs,
        compiler_params=pltpu.CompilerParams(vmem_limit_bytes=limit * MIB),
    )(meta, *args)


def places(meta, slab, reach):
    base = slab - reach
    even = meta[1]
    return pl.multiple_of(even * base, 8), pl.multiple_of((1 - even) * base, 8)


def gather_rows(meta, dst, p_own, recv_e, recv_o):
    slab, reach = p_own.shape[0], recv_e.shape[0]
    e_at, o_at = places(meta, slab, reach)
    dst[...] = p_own[...]
    dst[pl.ds(e_at, reach), :] += recv_e[...]
    dst[pl.ds(o_at, reach), :] += recv_o[...]


def offer(meta, src, send_e, send_o):
    slab, reach = src.shape[0], send_e.shape[0]
    e_at, o_at = places(meta, slab, reach)
    send_e[...] = src[pl.ds(e_at, reach), :]
    send_o[...] = src[pl.ds(o_at, reach), :]


def begin_kernel(meta, basis, send_e, send_o, keep, give):
    n = basis.shape[1]
    offer(meta, basis, send_e, send_o)
    gram = dot_t(basis[...], basis[...])
    share(meta, gram[: n // 2, :], gram[n // 2 :, :], keep, give)


def inverse_kernel(meta, mine, other, load, inv, y):
    n = inv.shape[0]
    inv[: n // 2, :], inv[n // 2 :, :] = shared(meta, mine[...], other[...])
    lane = lax.broadcasted_iota(jnp.int32, (1, n), 1)
    lanes = lax.broadcasted_iota(jnp.int32, (n, n), 1)

    def pick(row, k):
        return jnp.sum(jnp.where(lane == k, row, 0.0), axis=1, keepdims=True)

    def step(j, carry):
        k = 2 * j
        m = inv[...]
        col_a = jnp.sum(jnp.where(lanes == k, m, 0.0), axis=1, keepdims=True)
        col_b = jnp.sum(jnp.where(lanes == k + 1, m, 0.0), axis=1, keepdims=True)
        row_a = inv[pl.ds(k, 1), :]
        row_b = inv[pl.ds(k + 1, 1), :]
        a, b, d = pick(row_a, k), pick(row_a, k + 1), pick(row_b, k + 1)
        schur = d - b * (b / a)
        row_a = jnp.where(lane == k, 1.0, jnp.where(lane == k + 1, 0.0, row_a))
        row_b = jnp.where(lane == k, 0.0, jnp.where(lane == k + 1, 1.0, row_b))
        new_b = (row_b - (b / a) * row_a) / schur
        new_a = (row_a - b * new_b) / a
        m = jnp.where((lanes == k) | (lanes == k + 1), 0.0, m)
        inv[...] = m - col_a * new_a - col_b * new_b
        inv[pl.ds(k, 1), :] = new_a
        inv[pl.ds(k + 1, 1), :] = new_b
        return carry

    lax.fori_loop(0, n // 2, step, 0)
    y[...] = dot(inv[...], load[...])


def start_kernel(meta, p_own, recv_e, recv_o, rhs, y, c, r, send_e, send_o):
    gather_rows(meta, c, p_own, recv_e, recv_o)
    r[...] = rhs[...] - dot(c[...], y[...])
    offer(meta, r, send_e, send_o)


def share(meta, first, second, keep, give):
    n = first.shape[0]
    even = meta[1] == 1
    keep[:n, :] = jnp.where(even, first, second)
    give[:n, :] = jnp.where(even, second, first)


def shared(meta, mine, other):
    even = meta[1] == 1
    return jnp.where(even, mine, other), jnp.where(even, other, mine)


def pair_rows(meta, scalars, keep, give, n):
    even = meta[1] == 1
    keep[n:, :] = jnp.zeros((8, keep.shape[1]), F32)
    give[n:, :] = jnp.zeros((8, give.shape[1]), F32)
    for i, row in enumerate(scalars):
        keep[n + i : n + i + 1, :] = jnp.where(even, row, 0.0)
        give[n + i : n + i + 1, :] = jnp.where(even, 0.0, row)


def coarse_kernel(meta, basis, rhs, c, keep, give):
    share(meta, dot_t(basis[...], c[...]), dot_t(basis[...], rhs[...]), keep, give)


def amp_kernel(meta, mine, other, inverse, y, m, rho, amp):
    m_sum, b_sum = shared(meta, mine[...], other[...])
    coarse = b_sum - dot(m_sum, y[...])
    m[...] = m_sum
    rho[...] = coarse
    amp[...] = dot(inverse[...], coarse)


def image_kernel(meta, p_own, recv_e, recv_o, c, amp, w, send_e, send_o):
    gather_rows(meta, w, p_own, recv_e, recv_o)
    w[...] = w[...] - dot(c[...], amp[...])
    offer(meta, w, send_e, send_o)


def sums_kernel(meta, c, r, y, basis, amp, w, u, keep, give, lam):
    n = basis.shape[1]
    lam[...] = dot(basis[...], y[...])
    u[...] = r[...] - dot(basis[...], amp[...])
    share(meta, dot_t(c[...], u[...]), dot_t(c[...], w[...]), keep, give)
    pair_rows(meta, [total(u[...] * u[...]), total(u[...] * w[...])], keep, give, n)


def amp0_kernel(meta, mine, other, inverse, m, k0, a0, cq0, scal):
    n = inverse.shape[0]
    first, second = shared(meta, mine[...], other[...])
    amp = dot(inverse[...], first[:n, :])
    k0[...] = first[:n, :]
    a0[...] = amp
    cq0[...] = second[:n, :] - dot(m[...], amp)
    scal[...] = first[n:, :]


def first_kernel(meta, p_own, recv_e, recv_o, c, a0, scal, w, w1, send_e, send_o):
    gather_rows(meta, w1, p_own, recv_e, recv_o)
    alpha = scal[0:1, :] / scal[1:2, :]
    w1[...] = w[...] - alpha * (w1[...] - dot(c[...], a0[...]))
    offer(meta, w1, send_e, send_o)


def sums1_kernel(meta, basis, c, a0, k0, scal, u, w, lam, rho, p_own, recv_e, recv_o, w1,
                 lam1, u1, q0, rho1, keep, give, n0):
    n = basis.shape[1]
    gather_rows(meta, n0, p_own, recv_e, recv_o)
    alpha = scal[0:1, :] / scal[1:2, :]
    n0[...] = n0[...] - dot(c[...], a0[...])
    q0[...] = w[...] - dot(basis[...], a0[...])
    u1[...] = u[...] - alpha * q0[...]
    lam1[...] = lam[...] + alpha * u[...]
    rho1[...] = rho[...] - alpha * k0[...]
    share(meta, dot_t(c[...], u1[...]), dot_t(c[...], w1[...]), keep, give)
    pairs = ((u1, u1), (u1, w1), (u1, q0), (w1, w1), (w1, q0), (q0, q0), (n0, w1), (n0, q0))
    pair_rows(meta, [total(a[...] * b[...]) for a, b in pairs], keep, give, n)


def last_kernel(meta, mine, other, inverse, m, basis, u0, w1, u1, q0, lam1, rho1, k0, cq0, scal, lam, amp):
    n = inverse.shape[0]
    omega = total(mine[n + 8 :, :])
    first, second = shared(meta, mine[...], other[...])
    k1, l1 = first[:n, :], second[:n, :]
    uu, uw, uq, ww, wq, qq, nw, nq = (first[n + i : n + i + 1, :] for i in range(8))
    a1 = dot(inverse[...], k1)
    ma1 = dot(m[...], a1)
    beta = uu / scal[0:1, :]
    curve = uw + beta * (2.0 * uq + beta * scal[1:2, :])
    alpha = uu / curve
    mw = ww - total(a1 * k1)
    u_q1 = uw + beta * uq
    q1_q1 = mw + beta * (2.0 * wq + beta * qq)
    q1_w1 = mw + beta * wq
    m_n = nw - total(a1 * cq0[...])
    m_fm = omega + total(a1 * (ma1 - 2.0 * l1))
    q1_fq1 = m_fm + beta * (2.0 * m_n + beta * nq)
    gamma2 = uu + alpha * (alpha * q1_q1 - 2.0 * u_q1)
    delta2 = uw + alpha * (alpha * q1_fq1 - 2.0 * q1_w1)
    eps2 = u_q1 - alpha * q1_q1
    beta2 = gamma2 / uu
    p1 = u1[...] + beta * u0[...]
    q1 = w1[...] - dot(basis[...], a1) + beta * q0[...]
    curve2 = delta2 + beta2 * (2.0 * eps2 + beta2 * curve)
    alpha2 = gamma2 / curve2
    lam[...] = lam1[...] + alpha * p1 + alpha2 * (u1[...] - alpha * q1 + beta2 * p1)
    kk1 = k1 + beta * k0[...]
    k2 = k1 - alpha * (l1 - ma1 + beta * cq0[...])
    amp[...] = dot(inverse[...], rho1[...] - alpha * kk1 - alpha2 * (k2 + beta2 * kk1))


def steps(schur, offsets, rhs, basis, load):
    slab, cols = rhs.shape
    nc = basis.shape[1]
    reach = 3 * slab // 4
    index = lax.axis_index(AXES)
    meta = jnp.stack([offsets[0] - (slab - reach), 1 - index % 2]).astype(jnp.int32)
    vec, hal, sml = (slab, cols), (reach, cols), (nc, cols)
    rows8 = (8, cols)
    half = (nc + 8, cols)

    send_e, send_o, keep, give = call(
        begin_kernel, meta, (basis,), (hal, hal, (nc // 2, nc), (nc // 2, nc)))
    recv = swap(send_e, send_o)
    mine = near_sum(keep + core_swap(give))
    a_high, a_low = split(schur)
    mine = far_sum(mine)
    p_own, p_e, p_o = product(meta, a_high, a_low, (basis, *recv), True)
    recv = swap(p_e, p_o)
    other = core_swap(mine)
    inverse, y = call(inverse_kernel, meta, (mine, other, load), ((nc, nc), sml))
    c, r0, send_e, send_o = call(
        start_kernel, meta, (p_own, *recv, rhs, y), (vec, vec, hal, hal))
    recv = swap(send_e, send_o)
    keep, give = call(coarse_kernel, meta, (basis, rhs, c), (sml, sml))
    mine = near_sum(keep + core_swap(give))
    p_own, p_e, p_o = product(meta, a_high, a_low, (r0, *recv), True)
    recv = swap(p_e, p_o)
    mine = far_sum(mine)
    other = core_swap(mine)
    m, rho0, amp = call(amp_kernel, meta, (mine, other, inverse, y), (sml, sml, sml))
    w0, send_e, send_o = call(
        image_kernel, meta, (p_own, *recv, c, amp), (vec, hal, hal))
    recv = swap(send_e, send_o)
    u0, keep, give, lam0 = call(
        sums_kernel, meta, (c, r0, y, basis, amp, w0), (vec, half, half, vec))
    mine = near_sum(keep + core_swap(give))
    p_own, p_e, p_o = product(meta, a_high, a_low, (w0, *recv), True)
    recv = swap(p_e, p_o)
    mine = far_sum(mine)
    other = core_swap(mine)
    k0, a0, cq0, scal = call(
        amp0_kernel, meta, (mine, other, inverse, m), (sml, sml, sml, rows8))
    w1, send_e, send_o = call(
        first_kernel, meta, (p_own, *recv, c, a0, scal, w0), (vec, hal, hal))
    recv_in = swap(send_e, send_o)
    lam1, u1, q0, rho1, keep, give, _ = call(
        sums1_kernel, meta, (basis, c, a0, k0, scal, u0, w0, lam0, rho0, p_own, *recv, w1),
        (vec, vec, vec, sml, half, half, vec))
    mine = near_sum(keep + core_swap(give))
    (omega,) = product(meta, a_high, a_low, (w1, *recv_in), False)
    omega = near_sum(core_sum(omega))
    mine = far_sum(jnp.concatenate([mine, omega], axis=0))
    other = core_swap(mine)
    lam, amp = call(
        last_kernel, meta,
        (mine, other, inverse, m, basis, u0, w1, u1, q0, lam1, rho1, k0, cq0, scal),
        (vec, sml))
    return lam, amp


def solution(mesh):
    in_specs = (P(AXES, None, None), P(AXES), P(AXES, None), P(AXES, None), P())
    out_specs = (P(AXES, None), P())
    return jax.shard_map(steps, mesh=mesh, in_specs=in_specs, out_specs=out_specs, check_vma=False)
```
